32 devices in a mesh: row: 16 (over z, y, x), grp: 2 (over core).
Axes of the slice: x: 2, y: 2, z: 4, core: 2. Of those that a mesh axis runs over, the one named last changes fastest.
Arguments:
- features: float32 [131072, 256], P(('row', 'grp')), may hold values from -6 to 6
- session: int32 [131072], P(('row', 'grp')), may hold values from 0 to 1023, never falling along the last dimension, each value on 1 to 65536 neighbouring positions
- owner_map: int32 [32, 64], P(('row', 'grp')), may hold values from 0 to 15, as said below
Outputs:
- received: bfloat16 [4096, 64, 256], P(('row', 'grp'))
The draws below stay inside these ranges and needn't reach their ends.
Inputs may be any that keep to these rules, and one draw needn't show every extreme that they name: session numbers never fall along the rows; each session covers 1 to 65536 consecutive rows. `owner_map`: no owner is named by more than 8 of the blocks of one group of 64.
All inputs are finite; a program needn't handle non-finite values.
Results may differ from the reference program's by a relative error of at most 0.001.
Values may be sent and summed in bfloat16 or wider, within the bound.
No kernel may reach another device: no remote copies, remote signals or barrier semaphores. Data moves between devices by JAX's collectives and lax.ppermute only.
A program may use at most 128 MiB of HBM per device.

```python
import math
import jax
import jax.numpy as jnp
import numpy as np
from jax import lax

F = 256
BLOCK = 64
BLOCKS = 64
ROWS_DEV = 4096
ROWS = 131072
CAP = 8
SESSIONS = 1024
MOST = 65536
N_ROW = 16
N_GRP = 2
DEVICES = 32


def draw_owner_map(key, part):
    base = jax.random.fold_in(key, 11)
    key_pop, key_hot, key_noise, key_order = jax.random.split(base, 4)
    slot_capacity_total = N_ROW * CAP
    favored_devices = jax.random.randint(key_pop, (N_ROW,), 0, 96)
    busiest_device = jax.random.randint(key_hot, (), 0, N_ROW)
    candidate_owner = jnp.arange(slot_capacity_total) // CAP
    extra_reward = favored_devices[candidate_owner] + jnp.where(candidate_owner == busiest_device, 4096, 0)
    random_jitter = jax.random.randint(key_noise, (DEVICES, slot_capacity_total), 0, 64)
    owner_rating = (random_jitter + extra_reward[None, :]) * slot_capacity_total + jnp.arange(slot_capacity_total)[None, :]
    unused, picked = lax.top_k(owner_rating, BLOCKS)
    owners = candidate_owner[picked]
    shuffle = jax.random.randint(key_order, (DEVICES, BLOCKS), 0, 65536) * BLOCKS + jnp.arange(BLOCKS)[None, :]
    arrange = jnp.argsort(shuffle, axis=1)
    return jnp.take_along_axis(owners, arrange, axis=1).astype(jnp.int32)


def shard_levels(rng, dims, shards, low, largest):
    def one(position, parts):
        heights = jax.random.uniform(jax.random.fold_in(jax.random.fold_in(rng, 6), position), (parts,), jnp.float32, low / len(shards), largest / len(shards))
        return jnp.repeat(jnp.exp(heights), dims[position] // parts).reshape((-1,) + (1,) * (len(dims) - position - 1))

    gain = one(*shards[0])
    for cut in shards[1:]:
        gain = gain * one(*cut)
    return gain


def split_up(number_of, total, limit, lean):
    loads = [(1 << 20) // math.isqrt(rank ** lean) + 1 for rank in range(2, number_of + 1)]
    rest, counts = total - limit - (number_of - 1), [1] * (number_of - 1)
    while rest > 0:
        free = [i for i in range(number_of - 1) if counts[i] < limit]
        pool, remaining = sum([loads[i] for i in free]), rest
        for i in free:
            more = min(limit - counts[i], max(1, remaining * loads[i] // pool), rest)
            counts[i] = counts[i] + more
            rest = rest - more
    return np.array([limit] + counts)


def ragged_sizes(stream_key, number_of, total, limit, slope):
    if number_of == 2:
        one = jax.random.randint(stream_key, (), max(1, total - limit), min(limit, total - 1) + 1)
        return jnp.stack([one, total - one])
    lengths = jnp.asarray(split_up(number_of, total, limit, slope), jnp.int32)
    couples = (number_of - 1) // 2
    donor, receiver = lengths[1:1 + 2 * couples:2], lengths[2:2 + 2 * couples:2]
    slack = jnp.minimum(donor - 1, limit - receiver)
    shifted = jax.random.randint(jax.random.fold_in(stream_key, 1), (couples,), 0, 1 << 20) % (slack + 1)
    lengths = lengths.at[1:1 + 2 * couples:2].set(donor - shifted).at[2:2 + 2 * couples:2].set(receiver + shifted)
    return lengths[jax.random.permutation(jax.random.fold_in(stream_key, 2), number_of)]


def noise(key, shape, scale, most, pieces=(), dtype=jnp.bfloat16):
    values = jax.random.normal(key, shape, jnp.float32) * scale
    if len(pieces) > 0:
        values = shard_levels(key, shape, pieces, -0.22, 0.18) * values
    return jnp.clip(values, min=-most, max=most).astype(dtype)


def setup_inputs(seed: int = 0) -> dict:
    seeds = jax.random.split(jax.random.key(seed), 4)
    return {
        "features": noise(seeds[0], (ROWS, F), 1.0, 6.0, ((0, 32),), jnp.float32),
        "session": jnp.searchsorted(jnp.cumsum(ragged_sizes(seeds[1], SESSIONS, ROWS, MOST, 2)), jnp.arange(ROWS), side="right").astype(jnp.int32),
        "owner_map": draw_owner_map(jax.random.fold_in(seeds[3], 71), 0),
    }


def combine(earlier, latter):
    same_ids = earlier[0] == latter[0]
    return (latter[0], latter[1] + jnp.where(same_ids[..., None], earlier[1], 0.0), latter[2] + jnp.where(same_ids, earlier[2], 0.0))

def shard_step(carry, inputs):
    group_rows, group_ids = inputs
    all_ids = jnp.concatenate([carry[0][None], group_ids.astype(jnp.int32)])
    all_rows = jnp.concatenate([carry[1][None], group_rows])
    all_counts = jnp.concatenate([carry[2][None], jnp.ones((ROWS_DEV,), jnp.float32)])
    out_ids, out_rows, out_counts = lax.associative_scan(combine, (all_ids, all_rows, all_counts))
    normalized = (out_rows[1:] / jnp.sqrt(out_counts[1:])[:, None]).astype(jnp.bfloat16)
    return ((out_ids[-1], out_rows[-1], out_counts[-1]), normalized)

def reference(features, session, owner_map):
    grouped = features.reshape(DEVICES, ROWS_DEV, F)
    grouped_ids = session.reshape(DEVICES, ROWS_DEV)
    start = (jnp.array(-1, jnp.int32), jnp.zeros((F,), jnp.float32), jnp.array(0.0, jnp.float32))
    unused, normalized = lax.scan(shard_step, start, (grouped, grouped_ids))
    block_rows = normalized.reshape(DEVICES * BLOCKS, BLOCK, F)
    order = jnp.arange(BLOCKS).astype(jnp.int32)
    lower = order[None, :] < order[:, None]
    same_owner = owner_map[:, :, None] == owner_map[:, None, :]
    rank = lax.optimization_barrier(jnp.sum((same_owner & lower[None]).astype(jnp.int32), axis=2))
    device = jnp.arange(DEVICES).astype(jnp.int32)
    row_pos = device // N_GRP
    grp_pos = device % N_GRP
    target = (owner_map * N_GRP + grp_pos[:, None]) * (N_ROW * CAP) + row_pos[:, None] * CAP + rank
    received = jnp.zeros((DEVICES * N_ROW * CAP, BLOCK, F), jnp.bfloat16)
    received = received.at[target.reshape(-1).astype(jnp.int32)].set(block_rows)
    return received
```

```python
import functools

import jax
import jax.numpy as jnp
from jax import lax
from jax.experimental import pallas as pl
from jax.experimental.pallas import tpu as pltpu
from jax.sharding import PartitionSpec as P

LANES = 128
AXES = ("row", "grp")


def tail_kernel(ids_ref, x_ref, out_ref, acc_ref, *, rows):
    step = pl.program_id(0)
    chunk, width = x_ref.shape
    ids = ids_ref[...]
    id_rows = ids.shape[0]
    last = ids_ref[id_rows - 1 : id_rows, LANES - 1 : LANES]
    in_tail = jnp.where(ids == last, 1, 0)
    count = jnp.sum(jnp.sum(in_tail, axis=0, keepdims=True), axis=1, keepdims=True)

    @pl.when(step == 0)
    def _():
        acc_ref[...] = jnp.zeros_like(acc_ref)

    row = lax.broadcasted_iota(jnp.int32, (chunk, width), 0) + step * chunk
    kept = jnp.where(row >= rows - count, x_ref[...], 0.0)
    acc_ref[...] += jnp.sum(kept.reshape(chunk // 8, 8, width), axis=0)

    @pl.when(step == pl.num_programs(0) - 1)
    def _():
        copies = out_ref.shape[0]
        tail = jnp.sum(acc_ref[...], axis=0, keepdims=True)
        out_ref[:, :width] = jnp.broadcast_to(tail, (copies, width))
        lane = lax.broadcasted_iota(jnp.int32, (copies, LANES), 1)
        first = ids_ref[0:1, 0:1]
        meta = jnp.where(lane == 0, first, jnp.where(lane == 1, last, count))
        out_ref[:, width:] = meta.astype(jnp.float32)


def tails(ids, features, copies):
    rows, width = features.shape
    chunk = rows // 8
    return pl.pallas_call(
        functools.partial(tail_kernel, rows=rows),
        grid=(rows // chunk,),
        in_specs=[
            pl.BlockSpec(ids.shape, lambda i: (0, 0)),
            pl.BlockSpec((chunk, width), lambda i: (i, 0)),
        ],
        out_specs=pl.BlockSpec((copies, width + LANES), lambda i: (0, 0)),
        out_shape=jax.ShapeDtypeStruct((copies, width + LANES), jnp.float32),
        scratch_shapes=[pltpu.VMEM((8, width), jnp.float32)],
        name="tails",
    )(ids, features)


def blocks_kernel(
    here_ref, owners_ref, ids_ref, all_ref, x_ref, out_ref,
    norm_ref, zero_ref, sum_ref, count_ref, slot_ref, used_ref, sem, *, cap
):
    step = pl.program_id(0)
    chunk, width = x_ref.shape
    blocks, block_rows, _ = norm_ref.shape
    owners = out_ref.shape[0] // cap
    tile = LANES
    tiles = chunk // tile
    ids_rows = ids_ref.shape[0]

    @pl.when(step == 0)
    def _():
        zero_ref[...] = jnp.zeros_like(zero_ref)
        first = ids_ref[0:1, 0:1].astype(jnp.float32)
        device = lax.broadcasted_iota(jnp.int32, (all_ref.shape[0], 1), 0)
        feeds = (device < here_ref[0]) & (all_ref[:, width + 1 : width + 2] == first)
        sum_ref[...] = jnp.sum(jnp.where(feeds, all_ref[:, :width], 0.0), axis=0, keepdims=True)
        counts = jnp.where(feeds, all_ref[:, width + 2 : width + 3], 0.0)
        count_ref[...] = jnp.broadcast_to(jnp.sum(counts, axis=0, keepdims=True), count_ref.shape)

        @pl.loop(0, owners)
        def _(o):
            used_ref[o] = 0

        @pl.loop(0, blocks)
        def _(b):
            o = owners_ref[0, b]
            rank = used_ref[o]
            used_ref[o] = rank + 1
            slot_ref[b] = o * cap + rank

        @pl.loop(0, owners)
        def _(o):
            @pl.loop(used_ref[o], cap)
            def _(k):
                pltpu.make_async_copy(zero_ref, out_ref.at[o * cap + k], sem).start()

    lower = lax.broadcasted_iota(jnp.int32, (tile, tile), 1) <= lax.broadcasted_iota(
        jnp.int32, (tile, tile), 0
    )
    ones = jnp.ones((tile, LANES), jnp.bfloat16)
    row = lax.broadcasted_iota(jnp.int32, (tile, LANES), 0)
    carry = sum_ref[...]
    carry_count = count_ref[...]
    for k in range(tiles):
        t = step * tiles + k
        id_row = ids_ref[pl.ds(t, 1), :].astype(jnp.float32)
        before = ids_ref[pl.ds(jnp.maximum(t - 1, 0), 1), LANES - 1 : LANES].astype(jnp.float32)
        if k == 0:
            before = jnp.where(t == 0, id_row[:, :1], before)
        ids = jnp.broadcast_to(id_row, (tile, tile))
        same = (ids == ids.T) & lower
        mask = jnp.where(same, 1.0, 0.0).astype(jnp.bfloat16)
        x = x_ref[pl.ds(k * tile, tile), :]
        high = x.astype(jnp.bfloat16)
        rest = x - high.astype(jnp.float32)
        middle = rest.astype(jnp.bfloat16)
        low = (rest - middle.astype(jnp.float32)).astype(jnp.bfloat16)
        total = (
            jnp.dot(mask, low, preferred_element_type=jnp.float32)
            + jnp.dot(mask, middle, preferred_element_type=jnp.float32)
        ) + jnp.dot(mask, high, preferred_element_type=jnp.float32)
        count = jnp.dot(mask, ones, preferred_element_type=jnp.float32)
        joined = jnp.sum(jnp.where(id_row == before, 1, 0), axis=1, keepdims=True)
        follows = row < joined
        follows_wide = jnp.concatenate([follows] * (width // LANES), axis=1)
        total = total + jnp.where(follows_wide, carry, 0.0)
        count = count + jnp.where(follows, carry_count, 0.0)
        carry = total[tile - 1 :, :]
        carry_count = count[tile - 1 :, :]
        scale = lax.rsqrt(count)
        value = (total * jnp.concatenate([scale] * (width // LANES), axis=1)).astype(jnp.bfloat16)
        per_tile = tile // block_rows
        for p in range(per_tile):
            b = t * per_tile + p
            norm_ref[b] = value[p * block_rows : (p + 1) * block_rows, :]
            pltpu.make_async_copy(norm_ref.at[b], out_ref.at[slot_ref[b]], sem).start()
    sum_ref[...] = carry
    count_ref[...] = carry_count

    @pl.when(step == pl.num_programs(0) - 1)
    def _():
        pltpu.make_async_copy(out_ref, out_ref, sem).wait()


def slotted(here, owners, ids, everything, features, slots, cap):
    rows, width = features.shape
    blocks = owners.shape[1]
    block_rows = rows // blocks
    chunk = rows // 8
    return pl.pallas_call(
        functools.partial(blocks_kernel, cap=cap),
        grid=(rows // chunk,),
        in_specs=[
            pl.BlockSpec(memory_space=pltpu.SMEM),
            pl.BlockSpec(memory_space=pltpu.SMEM),
            pl.BlockSpec(ids.shape, lambda i: (0, 0)),
            pl.BlockSpec(everything.shape, lambda i: (0, 0)),
            pl.BlockSpec((chunk, width), lambda i: (i, 0)),
        ],
        out_specs=pl.BlockSpec(memory_space=pl.ANY),
        out_shape=jax.ShapeDtypeStruct((slots, block_rows, width), jnp.bfloat16),
        scratch_shapes=[
            pltpu.VMEM((blocks, block_rows, width), jnp.bfloat16),
            pltpu.VMEM((block_rows, width), jnp.bfloat16),
            pltpu.VMEM((1, width), jnp.float32),
            pltpu.VMEM((1, LANES), jnp.float32),
            pltpu.SMEM((blocks,), jnp.int32),
            pltpu.SMEM((slots // cap,), jnp.int32),
            pltpu.SemaphoreType.DMA,
        ],
        name="slotted",
    )(here, owners, ids, everything, features)


def body(features, session, owner_map):
    rows, _ = features.shape
    blocks = owner_map.shape[1]
    row_count, grp_count = lax.axis_size("row"), lax.axis_size("grp")
    cap = max(1, 2 * blocks // row_count)
    ids = session.reshape(rows // LANES, LANES)
    everything = lax.all_to_all(
        tails(ids, features, row_count * grp_count), AXES, split_axis=0, concat_axis=0, tiled=True
    )
    here = (lax.axis_index("row") * grp_count + lax.axis_index("grp")).reshape(1)
    outgoing = slotted(here, owner_map, ids, everything, features, row_count * cap, cap)
    return lax.all_to_all(outgoing, "row", split_axis=0, concat_axis=0, tiled=True)


def solution(mesh):
    in_specs = (P(AXES, None), P(AXES), P(AXES, None))
    return jax.shard_map(
        body, mesh=mesh, in_specs=in_specs, out_specs=P(AXES, None, None), check_vma=False
    )
```

```python
import functools

import jax
import jax.numpy as jnp
from jax import lax
from jax.experimental import pallas as pl
from jax.experimental.pallas import tpu as pltpu
from jax.sharding import PartitionSpec as P

LANES = 128
AXES = ("row", "grp")
PIECES = 8


def piece_copy(hbm_ref, vmem_ref, sem_ref, piece):
    rows = hbm_ref.shape[0] // PIECES
    part = pl.ds(pl.multiple_of(piece * rows, rows), rows)
    return pltpu.make_async_copy(hbm_ref.at[part], vmem_ref.at[part], sem_ref.at[piece])


def tail_kernel(ids_ref, x_hbm, out_ref, x_ref, sem_ref):
    rows, width = x_ref.shape
    chunk = rows // PIECES
    for piece in range(PIECES):
        piece_copy(x_hbm, x_ref, sem_ref, piece).start()
    ids = ids_ref[...]
    id_rows = ids.shape[0]
    last = ids_ref[id_rows - 1 : id_rows, LANES - 1 : LANES]
    in_tail = jnp.where(ids == last, 1, 0)
    count = jnp.sum(jnp.sum(in_tail, axis=0, keepdims=True), axis=1, keepdims=True)
    copies = out_ref.shape[0]
    lane = lax.broadcasted_iota(jnp.int32, (1, LANES), 1)
    meta = jnp.where(lane == 0, ids_ref[0:1, 0:1], jnp.where(lane == 1, last, count))
    row = lax.broadcasted_iota(jnp.int32, (chunk, width), 0)

    def add(piece, total):
        piece_copy(x_hbm, x_ref, sem_ref, piece).wait()
        part = x_ref[pl.ds(pl.multiple_of(piece * chunk, chunk), chunk), :]
        kept = jnp.where(row >= rows - count - piece * chunk, part, 0.0)
        return total + jnp.sum(kept.reshape(chunk // 8, 8, width), axis=0)

    total = lax.fori_loop(0, PIECES, add, jnp.zeros((8, width), jnp.float32))
    tail = jnp.sum(total, axis=0, keepdims=True)
    message = jnp.concatenate([tail, meta.astype(jnp.float32)], axis=1)
    out_ref[...] = jnp.broadcast_to(message[None], out_ref.shape)


def tails(ids, features, copies):
    rows, width = features.shape
    return pl.pallas_call(
        tail_kernel,
        in_specs=[
            pl.BlockSpec(memory_space=pltpu.VMEM),
            pl.BlockSpec(memory_space=pl.ANY),
        ],
        out_specs=pl.BlockSpec(memory_space=pltpu.VMEM),
        out_shape=jax.ShapeDtypeStruct((copies, 1, width + LANES), jnp.float32),
        scratch_shapes=[
            pltpu.VMEM((rows, width), jnp.float32),
            pltpu.SemaphoreType.DMA((PIECES,)),
        ],
        name="tails",
    )(ids, features)


def blocks_kernel(
    here_ref, owners_ref, ids_ref, all_ref, x_hbm, out_ref,
    x_ref, norm_ref, zero_ref, slot_ref, used_ref, sem_ref, sem, *, cap
):
    rows, width = x_ref.shape
    blocks, block_rows, _ = norm_ref.shape
    owners = out_ref.shape[0] // cap
    tile = LANES
    chunk = rows // PIECES
    tiles = chunk // tile
    for piece in range(PIECES):
        piece_copy(x_hbm, x_ref, sem_ref, piece).start()
    zero_ref[...] = jnp.zeros_like(zero_ref)

    @pl.loop(0, owners)
    def _(o):
        used_ref[o] = 0

    @pl.loop(0, blocks)
    def _(b):
        o = owners_ref[0, b]
        rank = used_ref[o]
        used_ref[o] = rank + 1
        slot_ref[b] = o * cap + rank

    @pl.loop(0, owners)
    def _(o):
        @pl.loop(used_ref[o], cap)
        def _(k):
            pltpu.make_async_copy(zero_ref, out_ref.at[o * cap + k], sem).start()

    everything = all_ref[:, 0, :]
    first = ids_ref[0:1, 0:1].astype(jnp.float32)
    device = lax.broadcasted_iota(jnp.int32, (everything.shape[0], 1), 0)
    feeds = (device < here_ref[0]) & (everything[:, width + 1 : width + 2] == first)
    carry = jnp.sum(jnp.where(feeds, everything[:, :width], 0.0), axis=0, keepdims=True)
    carry_count = jnp.sum(
        jnp.where(feeds, everything[:, width + 2 : width + 3], 0.0), axis=0, keepdims=True
    )
    carry_count = jnp.broadcast_to(carry_count, (1, LANES))

    lower = lax.broadcasted_iota(jnp.int32, (tile, tile), 1) <= lax.broadcasted_iota(
        jnp.int32, (tile, tile), 0
    )
    ones = jnp.ones((tile, LANES), jnp.bfloat16)
    row = lax.broadcasted_iota(jnp.int32, (tile, LANES), 0)

    def run(piece, carried):
        carry, carry_count, before = carried
        piece_copy(x_hbm, x_ref, sem_ref, piece).wait()
        for k in range(tiles):
            t = piece * tiles + k
            id_row = ids_ref[pl.ds(t, 1), :].astype(jnp.float32)
            ids = jnp.broadcast_to(id_row, (tile, tile))
            same = (ids == ids.T) & lower
            mask = jnp.where(same, 1.0, 0.0).astype(jnp.bfloat16)
            x = x_ref[pl.ds(pl.multiple_of(t * tile, tile), tile), :]
            high = x.astype(jnp.bfloat16)
            rest = x - high.astype(jnp.float32)
            middle = rest.astype(jnp.bfloat16)
            low = (rest - middle.astype(jnp.float32)).astype(jnp.bfloat16)
            total = (
                jnp.dot(mask, low, preferred_element_type=jnp.float32)
                + jnp.dot(mask, middle, preferred_element_type=jnp.float32)
            ) + jnp.dot(mask, high, preferred_element_type=jnp.float32)
            count = jnp.dot(mask, ones, preferred_element_type=jnp.float32)
            joined = jnp.sum(jnp.where(id_row == before, 1, 0), axis=1, keepdims=True)
            follows = row < joined
            follows_wide = jnp.concatenate([follows] * (width // LANES), axis=1)
            total = total + jnp.where(follows_wide, carry, 0.0)
            count = count + jnp.where(follows, carry_count, 0.0)
            carry = total[tile - 1 :, :]
            carry_count = count[tile - 1 :, :]
            before = id_row[:, LANES - 1 :]
            scale = lax.rsqrt(count)
            value = (total * jnp.concatenate([scale] * (width // LANES), axis=1)).astype(jnp.bfloat16)
            per_tile = tile // block_rows
            for p in range(per_tile):
                b = t * per_tile + p
                norm_ref[b] = value[p * block_rows : (p + 1) * block_rows, :]
                pltpu.make_async_copy(norm_ref.at[b], out_ref.at[slot_ref[b]], sem).start()
        return carry, carry_count, before

    lax.fori_loop(0, PIECES, run, (carry, carry_count, first))
    pltpu.make_async_copy(out_ref, out_ref, sem).wait()


def slotted(here, owners, ids, everything, features, slots, cap):
    rows, width = features.shape
    blocks = owners.shape[1]
    block_rows = rows // blocks
    return pl.pallas_call(
        functools.partial(blocks_kernel, cap=cap),
        in_specs=[
            pl.BlockSpec(memory_space=pltpu.SMEM),
            pl.BlockSpec(memory_space=pltpu.SMEM),
            pl.BlockSpec(memory_space=pltpu.VMEM),
            pl.BlockSpec(memory_space=pltpu.VMEM),
            pl.BlockSpec(memory_space=pl.ANY),
        ],
        out_specs=pl.BlockSpec(memory_space=pl.ANY),
        out_shape=jax.ShapeDtypeStruct((slots, block_rows, width), jnp.bfloat16),
        scratch_shapes=[
            pltpu.VMEM((rows, width), jnp.float32),
            pltpu.VMEM((blocks, block_rows, width), jnp.bfloat16),
            pltpu.VMEM((block_rows, width), jnp.bfloat16),
            pltpu.SMEM((blocks,), jnp.int32),
            pltpu.SMEM((slots // cap,), jnp.int32),
            pltpu.SemaphoreType.DMA((PIECES,)),
            pltpu.SemaphoreType.DMA,
        ],
        name="slotted",
    )(here, owners, ids, everything, features)


def body(features, session, owner_map):
    rows, _ = features.shape
    blocks = owner_map.shape[1]
    row_count, grp_count = lax.axis_size("row"), lax.axis_size("grp")
    cap = max(1, 2 * blocks // row_count)
    ids = session.reshape(rows // LANES, LANES)
    everything = lax.all_to_all(
        tails(ids, features, row_count * grp_count), AXES, split_axis=0, concat_axis=0, tiled=True
    )
    here = (lax.axis_index("row") * grp_count + lax.axis_index("grp")).reshape(1)
    outgoing = slotted(here, owner_map, ids, everything, features, row_count * cap, cap)
    return lax.all_to_all(outgoing, "row", split_axis=0, concat_axis=0, tiled=True)


def solution(mesh):
    in_specs = (P(AXES, None), P(AXES), P(AXES, None))
    return jax.shard_map(
        body, mesh=mesh, in_specs=in_specs, out_specs=P(AXES, None, None), check_vma=False
    )
```

```python
import functools

import jax
import jax.numpy as jnp
from jax import lax
from jax.experimental import pallas as pl
from jax.experimental.pallas import tpu as pltpu
from jax.sharding import PartitionSpec as P


LANES = 128
AXES = ("row", "grp")
PIECES = 8
VMEM = pl.BlockSpec(memory_space=pltpu.VMEM)
SMEM = pl.BlockSpec(memory_space=pltpu.SMEM)
ANY = pl.BlockSpec(memory_space=pl.ANY)
HBM = pl.BlockSpec(memory_space=pltpu.HBM)


def piece_copy(hbm_ref, vmem_ref, sem_ref, piece):
    rows = hbm_ref.shape[0] // PIECES
    part = pl.ds(pl.multiple_of(piece * rows, rows), rows)
    return pltpu.make_async_copy(hbm_ref.at[part], vmem_ref.at[part], sem_ref.at[piece])


def tail_kernel(place_ref, ids_ref, owners_ref, x_hbm, out_ref, x_ref, sem_ref, *, row_count, direct):
    rows, width = x_ref.shape
    chunk = rows // PIECES
    for piece in range(PIECES):
        piece_copy(x_hbm, x_ref, sem_ref, piece).start()
    ids = ids_ref[...]
    id_rows = ids.shape[0]
    last = ids_ref[id_rows - 1 : id_rows, LANES - 1 : LANES]
    in_tail = jnp.where(ids == last, 1, 0)
    count = jnp.sum(jnp.sum(in_tail, axis=0, keepdims=True), axis=1, keepdims=True)
    owners = owners_ref[...]
    blocks = owners.shape[1]
    owner = lax.broadcasted_iota(jnp.int32, (row_count, blocks), 0)
    sent = jnp.sum(jnp.where(owner == owners, 1, 0), axis=1, keepdims=True)
    half = max(1, row_count // 2)
    across = lax.broadcasted_iota(jnp.int32, (row_count, 1), 0) // half != place_ref[1] // half
    packed = jnp.sum(jnp.where(across, jnp.maximum(sent - direct, 0), 0), axis=0, keepdims=True)
    lane = lax.broadcasted_iota(jnp.int32, (1, LANES), 1)
    meta = jnp.where(lane == 2, count, packed)
    meta = jnp.where(lane == 0, ids_ref[0:1, 0:1], jnp.where(lane == 1, last, meta))
    row = lax.broadcasted_iota(jnp.int32, (chunk, width), 0)

    def add(piece, total):
        piece_copy(x_hbm, x_ref, sem_ref, piece).wait()
        part = x_ref[pl.ds(pl.multiple_of(piece * chunk, chunk), chunk), :]
        kept = jnp.where(row >= rows - count - piece * chunk, part, 0.0)
        return total + jnp.sum(kept.reshape(chunk // 8, 8, width), axis=0)

    total = lax.fori_loop(0, PIECES, add, jnp.zeros((8, width), jnp.float32))
    tail = jnp.sum(total, axis=0, keepdims=True)
    room = out_ref.shape[2] - width - LANES
    message = jnp.concatenate(
        [tail, meta.astype(jnp.float32), jnp.zeros((1, room), jnp.float32)], axis=1
    )
    out_ref[...] = jnp.broadcast_to(message[None], out_ref.shape)
    out_ref[:, :, width + LANES : width + LANES + blocks] = jnp.broadcast_to(
        owners.astype(jnp.float32)[None], (out_ref.shape[0], 1, blocks)
    )


def tails(place, ids, owners, features, copies, row_count, direct):
    rows, width = features.shape
    room = pl.cdiv(owners.shape[1], LANES) * LANES
    return pl.pallas_call(
        functools.partial(tail_kernel, row_count=row_count, direct=direct),
        in_specs=[SMEM, VMEM, VMEM, ANY],
        out_specs=VMEM,
        out_shape=jax.ShapeDtypeStruct((copies, 1, width + LANES + room), jnp.float32),
        scratch_shapes=[
            pltpu.VMEM((rows, width), jnp.float32),
            pltpu.SemaphoreType.DMA((PIECES,)),
        ],
        name="tails",
    )(place, ids, owners, features)


def place_blocks(owners_ref, used_ref, blocks, owner_count, put):
    @pl.loop(0, owner_count)
    def _(o):
        used_ref[o] = 0

    def one(b, packed):
        o = owners_ref[0, b]
        rank = used_ref[o]
        used_ref[o] = rank + 1
        return put(b, o, rank, packed)

    return lax.fori_loop(0, blocks, one, 0)


def blocks_kernel(
    place_ref, owners_ref, ids_ref, all_ref, x_hbm, *refs, owner_count, cap, direct, half
):
    outs, (x_ref, norm_ref, zero_ref, slot_ref, used_ref, sem_ref, done_ref) = refs[:-7], refs[-7:]
    rows, width = x_ref.shape
    blocks, block_rows, _ = norm_ref.shape
    tile = LANES
    chunk = rows // PIECES
    tiles = chunk // tile
    for piece in range(PIECES):
        piece_copy(x_hbm, x_ref, sem_ref, piece).start()
    zero_ref[...] = jnp.zeros_like(zero_ref)
    firsts = [0, half * cap, half * (cap + direct)]
    my_half = place_ref[1] // half
    me = place_ref[1] % half

    def put(b, o, rank, packed):
        local = o % half
        near = local * cap + rank
        if half == owner_count:
            slot_ref[b] = near
            return packed
        across = o // half != my_half
        over = across & (rank >= direct)
        far = firsts[1] + (local ^ me) * direct + rank
        slot_ref[b] = jnp.where(over, firsts[2] + packed, jnp.where(across, far, near))
        return packed + jnp.where(over, 1, 0)

    packed = place_blocks(owners_ref, used_ref, blocks, owner_count, put)

    def clear(kind, slot):
        pltpu.make_async_copy(zero_ref, outs[kind].at[slot], done_ref.at[kind]).start()

    @pl.loop(0, half)
    def _(o):
        @pl.loop(used_ref[my_half * half + o], cap)
        def _(k):
            clear(0, o * cap + k)

    if half < owner_count:
        @pl.loop(0, half)
        def _(o):
            @pl.loop(jnp.minimum(used_ref[(1 - my_half) * half + o], direct), direct)
            def _(k):
                clear(1, (o ^ me) * direct + k)

        @pl.loop(packed, outs[2].shape[0])
        def _(k):
            clear(2, k)

    def send(b):
        code = slot_ref[b]
        for kind in range(len(outs)):
            inside = code >= firsts[kind]
            if kind + 1 < len(outs):
                inside = inside & (code < firsts[kind + 1])

            @pl.when(inside)
            def _():
                pltpu.make_async_copy(
                    norm_ref.at[b], outs[kind].at[code - firsts[kind]], done_ref.at[kind]
                ).start()

    everything = all_ref[:, 0, :]
    first = ids_ref[0:1, 0:1].astype(jnp.float32)
    device = lax.broadcasted_iota(jnp.int32, (everything.shape[0], 1), 0)
    feeds = (device < place_ref[0]) & (everything[:, width + 1 : width + 2] == first)
    carry = jnp.sum(jnp.where(feeds, everything[:, :width], 0.0), axis=0, keepdims=True)
    carry_count = jnp.sum(
        jnp.where(feeds, everything[:, width + 2 : width + 3], 0.0), axis=0, keepdims=True
    )
    carry_count = jnp.broadcast_to(carry_count, (1, LANES))

    lower = lax.broadcasted_iota(jnp.int32, (tile, tile), 1) <= lax.broadcasted_iota(
        jnp.int32, (tile, tile), 0
    )
    ones = jnp.ones((tile, LANES), jnp.bfloat16)
    row = lax.broadcasted_iota(jnp.int32, (tile, LANES), 0)

    def run(piece, carried):
        carry, carry_count, before = carried
        piece_copy(x_hbm, x_ref, sem_ref, piece).wait()
        for k in range(tiles):
            t = piece * tiles + k
            id_row = ids_ref[pl.ds(t, 1), :].astype(jnp.float32)
            ids = jnp.broadcast_to(id_row, (tile, tile))
            same = (ids == ids.T) & lower
            mask = jnp.where(same, 1.0, 0.0).astype(jnp.bfloat16)
            x = x_ref[pl.ds(pl.multiple_of(t * tile, tile), tile), :]
            high = x.astype(jnp.bfloat16)
            rest = x - high.astype(jnp.float32)
            middle = rest.astype(jnp.bfloat16)
            low = (rest - middle.astype(jnp.float32)).astype(jnp.bfloat16)
            total = (
                jnp.dot(mask, low, preferred_element_type=jnp.float32)
                + jnp.dot(mask, middle, preferred_element_type=jnp.float32)
            ) + jnp.dot(mask, high, preferred_element_type=jnp.float32)
            count = jnp.dot(mask, ones, preferred_element_type=jnp.float32)
            joined = jnp.sum(jnp.where(id_row == before, 1, 0), axis=1, keepdims=True)
            follows = row < joined
            follows_wide = jnp.concatenate([follows] * (width // LANES), axis=1)
            total = total + jnp.where(follows_wide, carry, 0.0)
            count = count + jnp.where(follows, carry_count, 0.0)
            carry = total[tile - 1 :, :]
            carry_count = count[tile - 1 :, :]
            before = id_row[:, LANES - 1 :]
            scale = lax.rsqrt(count)
            value = (total * jnp.concatenate([scale] * (width // LANES), axis=1)).astype(jnp.bfloat16)
            per_tile = tile // block_rows
            for p in range(per_tile):
                b = t * per_tile + p
                norm_ref[b] = value[p * block_rows : (p + 1) * block_rows, :]
                send(b)
        return carry, carry_count, before

    lax.fori_loop(0, PIECES, run, (carry, carry_count, first))
    for kind, out in enumerate(outs):
        pltpu.make_async_copy(out, out, done_ref.at[kind]).wait()


def slotted(place, owners, ids, everything, features, owner_count, cap, direct, half, size):
    rows, width = features.shape
    blocks = owners.shape[1]
    block_rows = rows // blocks
    counts = [half * cap] + ([half * direct, size] if half < owner_count else [])
    return pl.pallas_call(
        functools.partial(
            blocks_kernel, owner_count=owner_count, cap=cap, direct=direct, half=half
        ),
        in_specs=[SMEM, SMEM, VMEM, VMEM, ANY],
        out_specs=[HBM] * len(counts),
        out_shape=[jax.ShapeDtypeStruct((n, block_rows, width), jnp.bfloat16) for n in counts],
        scratch_shapes=[
            pltpu.VMEM((rows, width), jnp.float32),
            pltpu.VMEM((blocks, block_rows, width), jnp.bfloat16),
            pltpu.VMEM((block_rows, width), jnp.bfloat16),
            pltpu.SMEM((blocks,), jnp.int32),
            pltpu.SMEM((owner_count,), jnp.int32),
            pltpu.SemaphoreType.DMA((PIECES,)),
            pltpu.SemaphoreType.DMA((3,)),
        ],
        name="slotted",
    )(place, owners, ids, everything, features)


def unpack_kernel(
    place_ref, owners_ref, packed_ref, out_ref, zero_ref, from_ref, used_ref, sem,
    *, owner_count, direct, half
):
    blocks = owners_ref.shape[1]
    extra = out_ref.shape[0] // half
    my_half = place_ref[1] // half
    zero_ref[...] = jnp.zeros_like(zero_ref)

    @pl.loop(0, half * extra)
    def _(s):
        from_ref[s] = -1

    def put(b, o, rank, packed):
        here = (rank >= direct) & (o // half == my_half)

        @pl.when(here)
        def _():
            from_ref[(o % half) * extra + rank - direct] = packed

        return packed + jnp.where(here, 1, 0)

    place_blocks(owners_ref, used_ref, blocks, owner_count, put)

    @pl.loop(0, half * extra)
    def _(s):
        source = from_ref[s]

        @pl.when(source >= 0)
        def _():
            pltpu.make_async_copy(packed_ref.at[jnp.maximum(source, 0)], out_ref.at[s], sem).start()

        @pl.when(source < 0)
        def _():
            pltpu.make_async_copy(zero_ref, out_ref.at[s], sem).start()

    pltpu.make_async_copy(out_ref, out_ref, sem).wait()


def unpack(place, owners, packed, owner_count, direct, half, extra):
    block_rows, width = packed.shape[1:]
    return pl.pallas_call(
        functools.partial(unpack_kernel, owner_count=owner_count, direct=direct, half=half),
        in_specs=[SMEM, SMEM, VMEM],
        out_specs=HBM,
        out_shape=jax.ShapeDtypeStruct((half * extra, block_rows, width), packed.dtype),
        scratch_shapes=[
            pltpu.VMEM((block_rows, width), jnp.bfloat16),
            pltpu.SMEM((half * extra,), jnp.int32),
            pltpu.SMEM((owner_count,), jnp.int32),
            pltpu.SemaphoreType.DMA,
        ],
        compiler_params=pltpu.CompilerParams(vmem_limit_bytes=8 << 20),
        name="unpack",
    )(place, owners, packed)


def gather_kernel(place_ref, near_ref, out_ref, sem, *, half):
    count = near_ref.shape[0]
    base = place_ref[1] // half * count
    copy = pltpu.make_async_copy(near_ref, out_ref.at[pl.ds(base, count)], sem)
    copy.start()
    copy.wait()


def gather(place, near, half):
    count, block_rows, width = near.shape
    return pl.pallas_call(
        functools.partial(gather_kernel, half=half),
        in_specs=[SMEM, VMEM],
        out_specs=HBM,
        out_shape=jax.ShapeDtypeStruct((2 * count, block_rows, width), near.dtype),
        scratch_shapes=[pltpu.SemaphoreType.DMA],
        compiler_params=pltpu.CompilerParams(vmem_limit_bytes=8 << 20),
        name="gather",
    )(place, near)


def finish_kernel(place_ref, proxied_ref, part_ref, *refs, half, cap, direct):
    far_refs, (out_ref, sem) = refs[:half], refs[half:]
    extra = cap - direct
    me = place_ref[1] % half
    base = (1 - place_ref[1] // half) * half
    for j in range(half):
        pltpu.make_async_copy(
            far_refs[j], out_ref.at[pl.ds((base + (me ^ j)) * cap, direct)], sem
        ).start()
        pltpu.make_async_copy(
            proxied_ref.at[pl.ds(j * extra, extra)],
            out_ref.at[pl.ds((base + j) * cap + direct, extra)],
            sem,
        ).start()
    part = out_ref.at[pl.ds(0, half * cap)]
    pltpu.make_async_copy(part, part, sem).wait()


def finish(place, proxied, out, fars, half, cap, direct):
    return pl.pallas_call(
        functools.partial(finish_kernel, half=half, cap=cap, direct=direct),
        in_specs=[SMEM, VMEM, HBM] + [VMEM] * half,
        out_specs=HBM,
        out_shape=jax.ShapeDtypeStruct(out.shape, out.dtype),
        input_output_aliases={2: 0},
        scratch_shapes=[pltpu.SemaphoreType.DMA],
        compiler_params=pltpu.CompilerParams(vmem_limit_bytes=8 << 20),
        name="finish",
    )(place, proxied, out, *fars)


def sizes_of(most):
    return sorted({max(1, most * k // 16) for k in SIZES} | {most})


SIZES = (7, 8, 9, 10, 12)


def body(features, session, owner_map):
    rows, width = features.shape
    blocks = owner_map.shape[1]
    row_count, grp_count = lax.axis_size("row"), lax.axis_size("grp")
    cap = max(1, 2 * blocks // row_count)
    split = cap > 1 and row_count > 2 and row_count & (row_count - 1) == 0
    half = row_count // 2 if split else row_count
    direct = cap * 4 // 8 if split else cap
    extra = cap - direct
    ids = session.reshape(rows // LANES, LANES)
    row, grp = lax.axis_index("row"), lax.axis_index("grp")
    place = jnp.stack([row * grp_count + grp, row])
    everything = lax.all_to_all(
        tails(place, ids, owner_map, features, row_count * grp_count, row_count, direct),
        AXES, split_axis=0, concat_axis=0, tiled=True,
    )
    if not split:
        (sent,) = slotted(
            place, owner_map, ids, everything, features, row_count, cap, direct, half, 0
        )
        return lax.all_to_all(sent, "row", split_axis=0, concat_axis=0, tiled=True)
    groups = [list(range(half)), list(range(half, row_count))]
    most = jnp.max(everything[:, 0, width + 3]).astype(jnp.int32)
    sizes = sizes_of(half * extra)

    def swap(j):
        return [(r, r ^ (half + j)) for r in range(row_count)]

    def exchange(x):
        return lax.all_to_all(
            x, "row", split_axis=0, concat_axis=0, tiled=True, axis_index_groups=groups
        )

    def branch(size):
        def run(place, owner_map, ids, everything, features):
            near, far, packed = slotted(
                place, owner_map, ids, everything, features, row_count, cap, direct, half, size
            )
            packed = lax.ppermute(packed, "row", swap(0))
            near = exchange(near)
            fars = []
            for j in range(half):
                part = far[j * direct : (j + 1) * direct]
                fars.append(lax.ppermute(part, "row", swap(j)))
            other = (place[1] ^ half) * grp_count + grp
            other_owners = lax.dynamic_slice(
                everything, (other, 0, width + LANES), (1, 1, blocks)
            ).reshape(1, blocks).astype(jnp.int32)
            proxied = unpack(place, other_owners, packed, row_count, direct, half, extra)
            proxied = exchange(proxied)
            out = gather(place, near, half)
            return finish(place, proxied, out, fars, half, cap, direct)

        return run

    which = sum((most > size).astype(jnp.int32) for size in sizes[:-1])
    return lax.switch(
        which, [branch(size) for size in sizes],
        place, owner_map, ids, everything, features,
    )


def solution(mesh):
    in_specs = (P(AXES, None), P(AXES), P(AXES, None))
    return jax.shard_map(
        body, mesh=mesh, in_specs=in_specs, out_specs=P(AXES, None, None), check_vma=False
    )
```

```python
import functools

import jax
import jax.numpy as jnp
from jax import lax
from jax.experimental import pallas as pl
from jax.experimental.pallas import tpu as pltpu
from jax.sharding import PartitionSpec as P


LANES = 128
AXES = ("row", "grp")
PIECES = 8
VMEM = pl.BlockSpec(memory_space=pltpu.VMEM)
SMEM = pl.BlockSpec(memory_space=pltpu.SMEM)
ANY = pl.BlockSpec(memory_space=pl.ANY)
HBM = pl.BlockSpec(memory_space=pltpu.HBM)


def piece_copy(hbm_ref, vmem_ref, sem_ref, piece):
    rows = hbm_ref.shape[0] // PIECES
    part = pl.ds(pl.multiple_of(piece * rows, rows), rows)
    return pltpu.make_async_copy(hbm_ref.at[part], vmem_ref.at[part], sem_ref.at[piece])


def here():
    row, grp = lax.axis_index("row"), lax.axis_index("grp")
    return row * lax.axis_size("grp") + grp, row


def loaded(copies):
    for copy in copies:
        copy.start()
    return copies


def column(row, size):
    return jnp.broadcast_to(row.astype(jnp.float32), (size, row.shape[1])).T.astype(jnp.int32)


def padded(row):
    return jnp.concatenate([row, jnp.zeros((1, LANES - row.shape[1]), row.dtype)], axis=1)


def tail_kernel(
    ids_hbm, owners_hbm, x_hbm, out_ref, table_ref, ids_ref, owners_ref, x_ref, sem_ref,
    *, row_count, cap, direct, half
):
    rows, width = x_ref.shape
    chunk = rows // PIECES
    small = loaded([
        pltpu.make_async_copy(ids_hbm, ids_ref, sem_ref.at[PIECES]),
        pltpu.make_async_copy(owners_hbm, owners_ref, sem_ref.at[PIECES + 1]),
    ])
    for piece in range(PIECES):
        piece_copy(x_hbm, x_ref, sem_ref, piece).start()
    my_row = here()[1]
    for copy in small:
        copy.wait()
    ids = ids_ref[...]
    id_rows = ids.shape[0]
    last = ids_ref[id_rows - 1 : id_rows, LANES - 1 : LANES]
    in_tail = jnp.where(ids == last, 1, 0)
    count = jnp.sum(jnp.sum(in_tail, axis=0, keepdims=True), axis=1, keepdims=True)

    blocks = owners_ref.shape[1]
    extra = cap - direct
    owners = padded(owners_ref[...])
    by_block = column(owners, LANES)
    block = lax.broadcasted_iota(jnp.int32, (LANES, LANES), 0)
    lane = lax.broadcasted_iota(jnp.int32, (LANES, LANES), 1)
    before = (block < lane) & (block < blocks)
    rank = jnp.sum(jnp.where(before & (by_block == owners), 1, 0), axis=0, keepdims=True)
    used = jnp.sum(jnp.where((by_block == lane) & (block < blocks), 1, 0), axis=0, keepdims=True)
    local = owners % half
    near = local * cap + rank
    if half < row_count:
        across = owners // half != my_row // half
        over = across & (rank >= direct) & (lane[:1] < blocks)
        over_by_block = column(jnp.where(over, 1, 0), LANES)
        packed = jnp.sum(jnp.where(before, over_by_block, 0), axis=0, keepdims=True)
        total_packed = jnp.sum(jnp.where(over, 1, 0), axis=1, keepdims=True)
        far = half * cap + (local ^ (my_row % half)) * direct + rank
        code = jnp.where(over, half * (cap + direct) + packed, jnp.where(across, far, near))
        goes = column(jnp.where(over, local * extra + rank - direct, -1), LANES)
        comes = jnp.where(goes == lane, column(packed, LANES) + 1, 0)
        source = jnp.sum(comes, axis=0, keepdims=True) - 1
    else:
        code, source, total_packed = near, rank, jnp.zeros_like(count)
    table_ref[0:1, :] = code
    table_ref[1:2, :] = used
    table_ref[2:3, :] = jnp.broadcast_to(total_packed, (1, LANES))

    lane = lane[:1]
    meta = jnp.where(lane == 2, count, total_packed)
    meta = jnp.where(lane == 0, ids_ref[0:1, 0:1], jnp.where(lane == 1, last, meta))
    row = lax.broadcasted_iota(jnp.int32, (chunk, width), 0)

    def add(piece, total):
        piece_copy(x_hbm, x_ref, sem_ref, piece).wait()
        part = x_ref[pl.ds(pl.multiple_of(piece * chunk, chunk), chunk), :]
        kept = jnp.where(row >= rows - count - piece * chunk, part, 0.0)
        return total + jnp.sum(kept.reshape(chunk // 8, 8, width), axis=0)

    total = lax.fori_loop(0, PIECES, add, jnp.zeros((8, width), jnp.float32))
    tail = jnp.sum(total, axis=0, keepdims=True)
    message = jnp.concatenate(
        [tail, meta.astype(jnp.float32), source.astype(jnp.float32)], axis=1
    )
    out_ref[...] = jnp.broadcast_to(message[None], out_ref.shape)


def tails(ids, owners, features, copies, row_count, cap, direct, half):
    rows, width = features.shape
    return pl.pallas_call(
        functools.partial(tail_kernel, row_count=row_count, cap=cap, direct=direct, half=half),
        in_specs=[ANY, ANY, ANY],
        out_specs=[VMEM, VMEM],
        out_shape=[
            jax.ShapeDtypeStruct((copies, 1, width + 2 * LANES), jnp.float32),
            jax.ShapeDtypeStruct((3, LANES), jnp.int32),
        ],
        scratch_shapes=[
            pltpu.VMEM(ids.shape, ids.dtype),
            pltpu.VMEM(owners.shape, owners.dtype),
            pltpu.VMEM((rows, width), jnp.float32),
            pltpu.SemaphoreType.DMA((PIECES + 2,)),
        ],
        name="tails",
    )(ids, owners, features)


def blocks_kernel(
    table_hbm, ids_hbm, all_hbm, x_hbm, *refs, owner_count, cap, direct, half
):
    outs, scratch = refs[:-8], refs[-8:]
    table_ref, ids_ref, all_ref, x_ref, norm_ref, zero_ref, sem_ref, done_ref = scratch
    rows, width = x_ref.shape
    _, block_rows, _ = norm_ref.shape
    tile = LANES
    chunk = rows // PIECES
    tiles = chunk // tile
    small = loaded([
        pltpu.make_async_copy(table_hbm, table_ref, sem_ref.at[PIECES]),
        pltpu.make_async_copy(ids_hbm, ids_ref, sem_ref.at[PIECES + 1]),
        pltpu.make_async_copy(all_hbm, all_ref, sem_ref.at[PIECES + 2]),
    ])
    for piece in range(PIECES):
        piece_copy(x_hbm, x_ref, sem_ref, piece).start()
    zero_ref[...] = jnp.zeros_like(zero_ref)
    firsts = [0, half * cap, half * (cap + direct)]
    my_device, my_row = here()
    my_half, me = my_row // half, my_row % half
    for copy in small:
        copy.wait()

    def clear(kind, slot):
        pltpu.make_async_copy(zero_ref, outs[kind].at[slot], done_ref.at[kind]).start()

    @pl.loop(0, half)
    def _(o):
        @pl.loop(table_ref[1, my_half * half + o], cap)
        def _(k):
            clear(0, o * cap + k)

    if half < owner_count:
        @pl.loop(0, half)
        def _(o):
            @pl.loop(jnp.minimum(table_ref[1, (1 - my_half) * half + o], direct), direct)
            def _(k):
                clear(1, (o ^ me) * direct + k)

        @pl.loop(table_ref[2, 0], outs[2].shape[0])
        def _(k):
            clear(2, k)

    def send(b):
        code = table_ref[0, b]
        for kind in range(len(outs)):
            inside = code >= firsts[kind]
            if kind + 1 < len(outs):
                inside = inside & (code < firsts[kind + 1])

            @pl.when(inside)
            def _():
                pltpu.make_async_copy(
                    norm_ref.at[b], outs[kind].at[code - firsts[kind]], done_ref.at[kind]
                ).start()

    everything = all_ref[:, 0, :]
    first = ids_ref[0:1, 0:1].astype(jnp.float32)
    device = lax.broadcasted_iota(jnp.int32, (everything.shape[0], 1), 0)
    feeds = (device < my_device) & (everything[:, width + 1 : width + 2] == first)
    carry = jnp.sum(jnp.where(feeds, everything[:, :width], 0.0), axis=0, keepdims=True)
    carry_count = jnp.sum(
        jnp.where(feeds, everything[:, width + 2 : width + 3], 0.0), axis=0, keepdims=True
    )
    carry_count = jnp.broadcast_to(carry_count, (1, LANES))

    lower = lax.broadcasted_iota(jnp.int32, (tile, tile), 1) <= lax.broadcasted_iota(
        jnp.int32, (tile, tile), 0
    )
    ones = jnp.ones((tile, LANES), jnp.bfloat16)
    row = lax.broadcasted_iota(jnp.int32, (tile, LANES), 0)

    def run(piece, carried):
        carry, carry_count, before = carried
        piece_copy(x_hbm, x_ref, sem_ref, piece).wait()
        for k in range(tiles):
            t = piece * tiles + k
            id_row = ids_ref[pl.ds(t, 1), :].astype(jnp.float32)
            ids = jnp.broadcast_to(id_row, (tile, tile))
            same = (ids == ids.T) & lower
            mask = jnp.where(same, 1.0, 0.0).astype(jnp.bfloat16)
            x = x_ref[pl.ds(pl.multiple_of(t * tile, tile), tile), :]
            high = x.astype(jnp.bfloat16)
            rest = x - high.astype(jnp.float32)
            middle = rest.astype(jnp.bfloat16)
            low = (rest - middle.astype(jnp.float32)).astype(jnp.bfloat16)
            count = jnp.dot(mask, ones, preferred_element_type=jnp.float32)
            twice = jnp.concatenate([mask, mask], axis=1)
            both = jnp.concatenate([high, middle], axis=0)
            total = jnp.dot(mask, low, preferred_element_type=jnp.float32) + jnp.dot(
                twice, both, preferred_element_type=jnp.float32
            )
            joined = jnp.sum(jnp.where(id_row == before, 1, 0), axis=1, keepdims=True)
            follows = row < joined
            follows_wide = jnp.concatenate([follows] * (width // LANES), axis=1)
            total = total + jnp.where(follows_wide, carry, 0.0)
            count = count + jnp.where(follows, carry_count, 0.0)
            carry = total[tile - 1 :, :]
            carry_count = count[tile - 1 :, :]
            before = id_row[:, LANES - 1 :]
            scale = lax.rsqrt(count)
            value = (total * jnp.concatenate([scale] * (width // LANES), axis=1)).astype(jnp.bfloat16)
            per_tile = tile // block_rows
            for p in range(per_tile):
                b = t * per_tile + p
                norm_ref[b] = value[p * block_rows : (p + 1) * block_rows, :]
                send(b)
        return carry, carry_count, before

    lax.fori_loop(0, PIECES, run, (carry, carry_count, first))
    for kind, out in enumerate(outs):
        pltpu.make_async_copy(out, out, done_ref.at[kind]).wait()


def slotted(table, ids, everything, features, blocks, owner_count, cap, direct, half, size):
    rows, width = features.shape
    block_rows = rows // blocks
    counts = [half * cap] + ([half * direct, size] if half < owner_count else [])
    return pl.pallas_call(
        functools.partial(
            blocks_kernel, owner_count=owner_count, cap=cap, direct=direct, half=half
        ),
        in_specs=[ANY] * 4,
        out_specs=[HBM] * len(counts),
        out_shape=[jax.ShapeDtypeStruct((n, block_rows, width), jnp.bfloat16) for n in counts],
        scratch_shapes=[
            pltpu.SMEM(table.shape, table.dtype),
            pltpu.VMEM(ids.shape, ids.dtype),
            pltpu.VMEM(everything.shape, everything.dtype),
            pltpu.VMEM((rows, width), jnp.float32),
            pltpu.VMEM((blocks, block_rows, width), jnp.bfloat16),
            pltpu.VMEM((block_rows, width), jnp.bfloat16),
            pltpu.SemaphoreType.DMA((PIECES + 3,)),
            pltpu.SemaphoreType.DMA((3,)),
        ],
        name="slotted",
    )(table, ids, everything, features)


def unpack_kernel(source_ref, packed_ref, out_ref, zero_ref, sem):
    zero_ref[...] = jnp.zeros_like(zero_ref)

    @pl.loop(0, out_ref.shape[0])
    def _(s):
        source = source_ref[0, s]

        @pl.when(source >= 0)
        def _():
            pltpu.make_async_copy(packed_ref.at[jnp.maximum(source, 0)], out_ref.at[s], sem).start()

        @pl.when(source < 0)
        def _():
            pltpu.make_async_copy(zero_ref, out_ref.at[s], sem).start()

    pltpu.make_async_copy(out_ref, out_ref, sem).wait()


def unpack(source, packed, count):
    block_rows, width = packed.shape[1:]
    return pl.pallas_call(
        unpack_kernel,
        in_specs=[SMEM, VMEM],
        out_specs=HBM,
        out_shape=jax.ShapeDtypeStruct((count, block_rows, width), packed.dtype),
        scratch_shapes=[
            pltpu.VMEM((block_rows, width), jnp.bfloat16),
            pltpu.SemaphoreType.DMA,
        ],
        compiler_params=pltpu.CompilerParams(vmem_limit_bytes=8 << 20),
        name="unpack",
    )(source, packed)


def gather_kernel(near_ref, out_ref, sem, *, half):
    count = near_ref.shape[0]
    base = here()[1] // half * count
    copy = pltpu.make_async_copy(near_ref, out_ref.at[pl.ds(base, count)], sem)
    copy.start()
    copy.wait()


def gather(near, half):
    count, block_rows, width = near.shape
    return pl.pallas_call(
        functools.partial(gather_kernel, half=half),
        in_specs=[VMEM],
        out_specs=HBM,
        out_shape=jax.ShapeDtypeStruct((2 * count, block_rows, width), near.dtype),
        scratch_shapes=[pltpu.SemaphoreType.DMA],
        compiler_params=pltpu.CompilerParams(vmem_limit_bytes=8 << 20),
        name="gather",
    )(near)


def finish_kernel(proxied_ref, part_ref, *refs, half, cap, direct):
    far_refs, (out_ref, sem) = refs[:half], refs[half:]
    extra = cap - direct
    my_row = here()[1]
    me = my_row % half
    base = (1 - my_row // half) * half
    for j in range(half):
        pltpu.make_async_copy(
            far_refs[j], out_ref.at[pl.ds((base + (me ^ j)) * cap, direct)], sem
        ).start()
        pltpu.make_async_copy(
            proxied_ref.at[pl.ds(j * extra, extra)],
            out_ref.at[pl.ds((base + j) * cap + direct, extra)],
            sem,
        ).start()
    part = out_ref.at[pl.ds(0, half * cap)]
    pltpu.make_async_copy(part, part, sem).wait()


def finish(proxied, out, fars, half, cap, direct):
    return pl.pallas_call(
        functools.partial(finish_kernel, half=half, cap=cap, direct=direct),
        in_specs=[VMEM, HBM] + [VMEM] * half,
        out_specs=HBM,
        out_shape=jax.ShapeDtypeStruct(out.shape, out.dtype),
        input_output_aliases={1: 0},
        scratch_shapes=[pltpu.SemaphoreType.DMA],
        compiler_params=pltpu.CompilerParams(vmem_limit_bytes=8 << 20),
        name="finish",
    )(proxied, out, *fars)


def sizes_of(most):
    return sorted({max(1, most * k // 16) for k in SIZES} | {most})


SIZES = (7, 8, 9, 10, 12)


def body(features, session, owner_map):
    rows, width = features.shape
    blocks = owner_map.shape[1]
    row_count, grp_count = lax.axis_size("row"), lax.axis_size("grp")
    cap = max(1, 2 * blocks // row_count)
    split = cap > 1 and row_count > 2 and row_count & (row_count - 1) == 0
    half = row_count // 2 if split else row_count
    direct = cap * 4 // 8 if split else cap
    extra = cap - direct
    ids = session.reshape(rows // LANES, LANES)
    row, grp = lax.axis_index("row"), lax.axis_index("grp")
    message, table = tails(
        ids, owner_map, features, row_count * grp_count, row_count, cap, direct, half
    )
    everything = lax.all_to_all(message, AXES, split_axis=0, concat_axis=0, tiled=True)
    if not split:
        (sent,) = slotted(
            table, ids, everything, features, blocks, row_count, cap, direct, half, 0
        )
        return lax.all_to_all(sent, "row", split_axis=0, concat_axis=0, tiled=True)
    groups = [list(range(half)), list(range(half, row_count))]
    most = jnp.max(everything[:, 0, width + 3]).astype(jnp.int32)
    sizes = sizes_of(half * extra)

    def swap(j):
        return [(r, r ^ (half + j)) for r in range(row_count)]

    def exchange(x):
        return lax.all_to_all(
            x, "row", split_axis=0, concat_axis=0, tiled=True, axis_index_groups=groups
        )

    def branch(size):
        def run(table, ids, everything, features):
            near, far, packed = slotted(
                table, ids, everything, features, blocks, row_count, cap, direct, half, size
            )
            packed = lax.ppermute(packed, "row", swap(0))
            near = exchange(near)
            fars = []
            for j in range(half):
                part = far[j * direct : (j + 1) * direct]
                fars.append(lax.ppermute(part, "row", swap(j)))
            other = (row ^ half) * grp_count + grp
            source = lax.dynamic_slice(
                everything, (other, 0, width + LANES), (1, 1, half * extra)
            ).reshape(1, half * extra).astype(jnp.int32)
            proxied = unpack(source, packed, half * extra)
            proxied = exchange(proxied)
            out = gather(near, half)
            return finish(proxied, out, fars, half, cap, direct)

        return run

    which = sum((most > size).astype(jnp.int32) for size in sizes[:-1])
    return lax.switch(
        which, [branch(size) for size in sizes],
        table, ids, everything, features,
    )


def solution(mesh):
    in_specs = (P(AXES, None), P(AXES), P(AXES, None))
    return jax.shard_map(
        body, mesh=mesh, in_specs=in_specs, out_specs=P(AXES, None, None), check_vma=False
    )
```

```python
import functools

import jax
import jax.numpy as jnp
from jax import lax
from jax.experimental import pallas as pl
from jax.experimental.pallas import tpu as pltpu
from jax.sharding import PartitionSpec as P


LANES = 128
AXES = ("row", "grp")
PIECES = 4
VMEM = pl.BlockSpec(memory_space=pltpu.VMEM)
SMEM = pl.BlockSpec(memory_space=pltpu.SMEM)
ANY = pl.BlockSpec(memory_space=pl.ANY)
HBM = pl.BlockSpec(memory_space=pltpu.HBM)


def piece_copy(hbm_ref, vmem_ref, sem_ref, piece):
    rows = hbm_ref.shape[0] // PIECES
    part = pl.ds(pl.multiple_of(piece * rows, rows), rows)
    return pltpu.make_async_copy(hbm_ref.at[part], vmem_ref.at[part], sem_ref.at[piece])


def here():
    row, grp = lax.axis_index("row"), lax.axis_index("grp")
    return row * lax.axis_size("grp") + grp, row


def loaded(copies):
    for copy in copies:
        copy.start()
    return copies


def column(row, size):
    return jnp.broadcast_to(row.astype(jnp.float32), (size, row.shape[1])).T.astype(jnp.int32)


def padded(row):
    return jnp.concatenate([row, jnp.zeros((1, LANES - row.shape[1]), row.dtype)], axis=1)


def tail_kernel(
    ids_hbm, owners_hbm, x_hbm, out_ref, table_ref, ids_ref, owners_ref, x_ref, sem_ref,
    *, row_count, cap, direct, half
):
    rows, width = x_ref.shape
    chunk = rows // PIECES
    small = loaded([
        pltpu.make_async_copy(ids_hbm, ids_ref, sem_ref.at[PIECES]),
        pltpu.make_async_copy(owners_hbm, owners_ref, sem_ref.at[PIECES + 1]),
    ])
    for piece in range(PIECES):
        piece_copy(x_hbm, x_ref, sem_ref, piece).start()
    my_row = here()[1]
    for copy in small:
        copy.wait()
    ids = ids_ref[...]
    id_rows = ids.shape[0]
    last = ids_ref[id_rows - 1 : id_rows, LANES - 1 : LANES]
    in_tail = jnp.where(ids == last, 1, 0)
    count = jnp.sum(jnp.sum(in_tail, axis=0, keepdims=True), axis=1, keepdims=True)

    blocks = owners_ref.shape[1]
    extra = cap - direct
    owners = padded(owners_ref[...])
    by_block = column(owners, LANES)
    block = lax.broadcasted_iota(jnp.int32, (LANES, LANES), 0)
    lane = lax.broadcasted_iota(jnp.int32, (LANES, LANES), 1)
    before = (block < lane) & (block < blocks)
    rank = jnp.sum(jnp.where(before & (by_block == owners), 1, 0), axis=0, keepdims=True)
    used = jnp.sum(jnp.where((by_block == lane) & (block < blocks), 1, 0), axis=0, keepdims=True)
    local = owners % half
    near = local * cap + rank
    if half < row_count:
        across = owners // half != my_row // half
        over = across & (rank >= direct) & (lane[:1] < blocks)
        over_by_block = column(jnp.where(over, 1, 0), LANES)
        packed = jnp.sum(jnp.where(before, over_by_block, 0), axis=0, keepdims=True)
        total_packed = jnp.sum(jnp.where(over, 1, 0), axis=1, keepdims=True)
        far = half * cap + (local ^ (my_row % half)) * direct + rank
        code = jnp.where(over, half * (cap + direct) + packed, jnp.where(across, far, near))
        goes = column(jnp.where(over, local * extra + rank - direct, -1), LANES)
        comes = jnp.where(goes == lane, column(packed, LANES) + 1, 0)
        source = jnp.sum(comes, axis=0, keepdims=True) - 1
    else:
        code, source, total_packed = near, rank, jnp.zeros_like(count)
    table_ref[0:1, :] = code
    table_ref[1:2, :] = used
    table_ref[2:3, :] = jnp.broadcast_to(total_packed, (1, LANES))

    lane = lane[:1]
    meta = jnp.where(lane == 2, count, total_packed)
    meta = jnp.where(lane == 0, ids_ref[0:1, 0:1], jnp.where(lane == 1, last, meta))
    row = lax.broadcasted_iota(jnp.int32, (chunk, width), 0)

    def add(piece, total):
        piece_copy(x_hbm, x_ref, sem_ref, piece).wait()
        part = x_ref[pl.ds(pl.multiple_of(piece * chunk, chunk), chunk), :]
        kept = jnp.where(row >= rows - count - piece * chunk, part, 0.0)
        return total + jnp.sum(kept.reshape(chunk // 8, 8, width), axis=0)

    total = lax.fori_loop(0, PIECES, add, jnp.zeros((8, width), jnp.float32))
    tail = jnp.sum(total, axis=0, keepdims=True)
    message = jnp.concatenate(
        [tail, meta.astype(jnp.float32), source.astype(jnp.float32)], axis=1
    )
    out_ref[...] = jnp.broadcast_to(message[None], out_ref.shape)


def tails(ids, owners, features, copies, row_count, cap, direct, half):
    rows, width = features.shape
    return pl.pallas_call(
        functools.partial(tail_kernel, row_count=row_count, cap=cap, direct=direct, half=half),
        in_specs=[ANY, ANY, ANY],
        out_specs=[VMEM, VMEM],
        out_shape=[
            jax.ShapeDtypeStruct((copies, 1, width + 2 * LANES), jnp.float32),
            jax.ShapeDtypeStruct((3, LANES), jnp.int32),
        ],
        scratch_shapes=[
            pltpu.VMEM(ids.shape, ids.dtype),
            pltpu.VMEM(owners.shape, owners.dtype),
            pltpu.VMEM((rows, width), jnp.float32),
            pltpu.SemaphoreType.DMA((PIECES + 2,)),
        ],
        name="tails",
    )(ids, owners, features)


def blocks_kernel(
    table_hbm, ids_hbm, all_hbm, x_hbm, *refs, owner_count, cap, direct, half
):
    outs, scratch = refs[:-8], refs[-8:]
    table_ref, ids_ref, all_ref, x_ref, norm_ref, zero_ref, sem_ref, done_ref = scratch
    rows, width = x_ref.shape
    _, block_rows, _ = norm_ref.shape
    tile = LANES
    chunk = rows // PIECES
    tiles = chunk // tile
    small = loaded([
        pltpu.make_async_copy(table_hbm, table_ref, sem_ref.at[PIECES]),
        pltpu.make_async_copy(ids_hbm, ids_ref, sem_ref.at[PIECES + 1]),
        pltpu.make_async_copy(all_hbm, all_ref, sem_ref.at[PIECES + 2]),
    ])
    for piece in range(PIECES):
        piece_copy(x_hbm, x_ref, sem_ref, piece).start()
    zero_ref[...] = jnp.zeros_like(zero_ref)
    firsts = [0, half * cap, half * (cap + direct)]
    my_device, my_row = here()
    my_half, me = my_row // half, my_row % half
    for copy in small:
        copy.wait()

    def clear(kind, slot):
        pltpu.make_async_copy(zero_ref, outs[kind].at[slot], done_ref.at[kind]).start()

    @pl.loop(0, half)
    def _(o):
        @pl.loop(table_ref[1, my_half * half + o], cap)
        def _(k):
            clear(0, o * cap + k)

    if half < owner_count:
        @pl.loop(0, half)
        def _(o):
            @pl.loop(jnp.minimum(table_ref[1, (1 - my_half) * half + o], direct), direct)
            def _(k):
                clear(1, (o ^ me) * direct + k)

        @pl.loop(table_ref[2, 0], outs[2].shape[0])
        def _(k):
            clear(2, k)

    def send(b):
        code = table_ref[0, b]
        for kind in range(len(outs)):
            inside = code >= firsts[kind]
            if kind + 1 < len(outs):
                inside = inside & (code < firsts[kind + 1])

            @pl.when(inside)
            def _():
                pltpu.make_async_copy(
                    norm_ref.at[b], outs[kind].at[code - firsts[kind]], done_ref.at[kind]
                ).start()

    everything = all_ref[:, 0, :]
    first = ids_ref[0:1, 0:1].astype(jnp.float32)
    device = lax.broadcasted_iota(jnp.int32, (everything.shape[0], 1), 0)
    feeds = (device < my_device) & (everything[:, width + 1 : width + 2] == first)
    carry = jnp.sum(jnp.where(feeds, everything[:, :width], 0.0), axis=0, keepdims=True)
    carry_count = jnp.sum(
        jnp.where(feeds, everything[:, width + 2 : width + 3], 0.0), axis=0, keepdims=True
    )
    carry_count = jnp.broadcast_to(carry_count, (1, LANES))

    lower = lax.broadcasted_iota(jnp.int32, (tile, tile), 1) <= lax.broadcasted_iota(
        jnp.int32, (tile, tile), 0
    )
    ones = jnp.ones((tile, LANES), jnp.bfloat16)
    row = lax.broadcasted_iota(jnp.int32, (tile, LANES), 0)

    def run(piece, carried):
        carry, carry_count, before = carried
        piece_copy(x_hbm, x_ref, sem_ref, piece).wait()
        for k in range(tiles):
            t = piece * tiles + k
            id_row = ids_ref[pl.ds(t, 1), :].astype(jnp.float32)
            ids = jnp.broadcast_to(id_row, (tile, tile))
            same = (ids == ids.T) & lower
            mask = jnp.where(same, 1.0, 0.0).astype(jnp.bfloat16)
            x = x_ref[pl.ds(pl.multiple_of(t * tile, tile), tile), :]
            high = x.astype(jnp.bfloat16)
            rest = x - high.astype(jnp.float32)
            middle = rest.astype(jnp.bfloat16)
            low = (rest - middle.astype(jnp.float32)).astype(jnp.bfloat16)
            count = jnp.dot(mask, ones, preferred_element_type=jnp.float32)
            twice = jnp.concatenate([mask, mask], axis=1)
            both = jnp.concatenate([high, middle], axis=0)
            total = jnp.dot(mask, low, preferred_element_type=jnp.float32) + jnp.dot(
                twice, both, preferred_element_type=jnp.float32
            )
            joined = jnp.sum(jnp.where(id_row == before, 1, 0), axis=1, keepdims=True)
            follows = row < joined
            follows_wide = jnp.concatenate([follows] * (width // LANES), axis=1)
            total = total + jnp.where(follows_wide, carry, 0.0)
            count = count + jnp.where(follows, carry_count, 0.0)
            carry = total[tile - 1 :, :]
            carry_count = count[tile - 1 :, :]
            before = id_row[:, LANES - 1 :]
            scale = lax.rsqrt(count)
            value = (total * jnp.concatenate([scale] * (width // LANES), axis=1)).astype(jnp.bfloat16)
            per_tile = tile // block_rows
            for p in range(per_tile):
                b = t * per_tile + p
                norm_ref[b] = value[p * block_rows : (p + 1) * block_rows, :]
                send(b)
        return carry, carry_count, before

    lax.fori_loop(0, PIECES, run, (carry, carry_count, first))
    for kind, out in enumerate(outs):
        pltpu.make_async_copy(out, out, done_ref.at[kind]).wait()


def slotted(table, ids, everything, features, blocks, owner_count, cap, direct, half, size):
    rows, width = features.shape
    block_rows = rows // blocks
    counts = [half * cap] + ([half * direct, size] if half < owner_count else [])
    return pl.pallas_call(
        functools.partial(
            blocks_kernel, owner_count=owner_count, cap=cap, direct=direct, half=half
        ),
        in_specs=[ANY] * 4,
        out_specs=[HBM] * len(counts),
        out_shape=[jax.ShapeDtypeStruct((n, block_rows, width), jnp.bfloat16) for n in counts],
        scratch_shapes=[
            pltpu.SMEM(table.shape, table.dtype),
            pltpu.VMEM(ids.shape, ids.dtype),
            pltpu.VMEM(everything.shape, everything.dtype),
            pltpu.VMEM((rows, width), jnp.float32),
            pltpu.VMEM((blocks, block_rows, width), jnp.bfloat16),
            pltpu.VMEM((block_rows, width), jnp.bfloat16),
            pltpu.SemaphoreType.DMA((PIECES + 3,)),
            pltpu.SemaphoreType.DMA((3,)),
        ],
        name="slotted",
    )(table, ids, everything, features)


def unpack_kernel(source_ref, packed_ref, out_ref):
    @pl.loop(0, out_ref.shape[0])
    def _(s):
        source = source_ref[0, s]
        block = packed_ref[jnp.maximum(source, 0)]
        out_ref[s] = jnp.where(source >= 0, block, jnp.zeros_like(block))


def unpack(source, packed, count):
    block_rows, width = packed.shape[1:]
    return pl.pallas_call(
        unpack_kernel,
        in_specs=[SMEM, VMEM],
        out_specs=VMEM,
        out_shape=jax.ShapeDtypeStruct((count, block_rows, width), packed.dtype),
        compiler_params=pltpu.CompilerParams(vmem_limit_bytes=8 << 20),
        name="unpack",
    )(source, packed)


def gather_kernel(near_ref, out_ref, sem, *, half):
    count = near_ref.shape[0]
    base = here()[1] // half * count
    copy = pltpu.make_async_copy(near_ref, out_ref.at[pl.ds(base, count)], sem)
    copy.start()
    copy.wait()


def gather(near, half):
    count, block_rows, width = near.shape
    return pl.pallas_call(
        functools.partial(gather_kernel, half=half),
        in_specs=[VMEM],
        out_specs=HBM,
        out_shape=jax.ShapeDtypeStruct((2 * count, block_rows, width), near.dtype),
        scratch_shapes=[pltpu.SemaphoreType.DMA],
        compiler_params=pltpu.CompilerParams(vmem_limit_bytes=8 << 20),
        name="gather",
    )(near)


def finish_kernel(part_ref, *refs, half, cap, direct, classes, proxied):
    far_refs, (out_ref, sem) = refs[:-2], refs[-2:]
    extra = cap - direct
    my_row = here()[1]
    me = my_row % half
    base = (1 - my_row // half) * half
    blocks = len(classes) * direct
    for j, far_ref in zip(classes, far_refs):
        pltpu.make_async_copy(
            far_ref, out_ref.at[pl.ds((base + (me ^ j)) * cap, direct)], sem
        ).start()
    if proxied:
        blocks += half * extra
        for j in range(half):
            pltpu.make_async_copy(
                far_refs[-1].at[pl.ds(j * extra, extra)],
                out_ref.at[pl.ds((base + j) * cap + direct, extra)],
                sem,
            ).start()
    part = out_ref.at[pl.ds(0, blocks)]
    pltpu.make_async_copy(part, part, sem).wait()


def finish(out, fars, classes, proxied, half, cap, direct):
    arrays = [fars[j] for j in classes] + ([] if proxied is None else [proxied])
    return pl.pallas_call(
        functools.partial(
            finish_kernel, half=half, cap=cap, direct=direct, classes=classes,
            proxied=proxied is not None,
        ),
        in_specs=[HBM] + [VMEM] * len(arrays),
        out_specs=HBM,
        out_shape=jax.ShapeDtypeStruct(out.shape, out.dtype),
        input_output_aliases={0: 0},
        scratch_shapes=[pltpu.SemaphoreType.DMA],
        compiler_params=pltpu.CompilerParams(vmem_limit_bytes=8 << 20),
        name="finish",
    )(out, *arrays)


def sizes_of(most):
    return sorted({max(1, most * k // 32) for k in SIZES} | {most})


LATE = 3
SIZES = (14, 15, 16, 17, 18, 19, 21, 25)


def body(features, session, owner_map):
    rows, width = features.shape
    blocks = owner_map.shape[1]
    row_count, grp_count = lax.axis_size("row"), lax.axis_size("grp")
    cap = max(1, 2 * blocks // row_count)
    split = cap > 1 and row_count > 2 and row_count & (row_count - 1) == 0
    half = row_count // 2 if split else row_count
    direct = cap * 4 // 8 if split else cap
    extra = cap - direct
    ids = session.reshape(rows // LANES, LANES)
    row, grp = lax.axis_index("row"), lax.axis_index("grp")
    message, table = tails(
        ids, owner_map, features, row_count * grp_count, row_count, cap, direct, half
    )
    everything = lax.all_to_all(message, AXES, split_axis=0, concat_axis=0, tiled=True)
    if not split:
        (sent,) = slotted(
            table, ids, everything, features, blocks, row_count, cap, direct, half, 0
        )
        return lax.all_to_all(sent, "row", split_axis=0, concat_axis=0, tiled=True)
    groups = [list(range(half)), list(range(half, row_count))]
    most = jnp.max(everything[:, 0, width : width + LANES], axis=0)[3].astype(jnp.int32)
    sizes = sizes_of(half * extra)

    def swap(j):
        return [(r, r ^ (half + j)) for r in range(row_count)]

    def exchange(x):
        return lax.all_to_all(
            x, "row", split_axis=0, concat_axis=0, tiled=True, axis_index_groups=groups
        )

    def branch(size):
        def run(table, ids, everything, features):
            near, far, packed = slotted(
                table, ids, everything, features, blocks, row_count, cap, direct, half, size
            )
            packed = lax.ppermute(packed, "row", swap(0))
            near = exchange(near)
            fars = []
            for j in range(half):
                part = far[j * direct : (j + 1) * direct]
                fars.append(lax.ppermute(part, "row", swap(j)))
            other = (row ^ half) * grp_count + grp
            source = lax.dynamic_slice(
                everything, (other, 0, width + LANES), (1, 1, half * extra)
            ).reshape(1, half * extra).astype(jnp.int32)
            proxied = unpack(source, packed, half * extra)
            proxied = exchange(proxied)
            out = gather(near, half)
            late = tuple(range(LATE))
            out = finish(out, fars, tuple(range(LATE, half)), None, half, cap, direct)
            return finish(out, fars, late, proxied, half, cap, direct)

        return run

    which = sum((most > size).astype(jnp.int32) for size in sizes[:-1])
    return lax.switch(
        which, [branch(size) for size in sizes],
        table, ids, everything, features,
    )


def solution(mesh):
    in_specs = (P(AXES, None), P(AXES), P(AXES, None))
    return jax.shard_map(
        body, mesh=mesh, in_specs=in_specs, out_specs=P(AXES, None, None), check_vma=False
    )
```
